256 devices in a mesh: gx: 32 (over z, y), gy: 8 (over x, core).
Axes of the slice: x: 4, y: 4, z: 8, core: 2. Of those that a mesh axis runs over, the one named last changes fastest.
Arguments:
- image_feats: bfloat16 [65536, 4096], P('gx', 'gy'), may hold values from -6 to 6
- w_kv: bfloat16 [4096, 2048], P('gy'), may hold values from -0.09375 to 0.09375
- k_gain: float32 [128], replicated, may hold values from 0.25 to 1.75
- tile_rows: int32 [512], replicated, may hold values from 0 to 128
- deal: int32 [32, 16], replicated, may hold values from 0 to 511, as said below
Outputs:
- keys_out: bfloat16 [65536, 1024], P('gx', 'gy')
- values_out: bfloat16 [65536, 1024], P('gx', 'gy')
The draws below stay inside these ranges and needn't reach their ends.
Inputs may be any that keep to these rules, and one draw needn't show every extreme that they name: Each input tile is named exactly once; deal[j, s] % 16 == s; two entries of one row j that name tiles of the same index of gx stand in columns s that differ by a multiple of 32, so one row names at most 1 tiles of one index of gx, and exactly 1 for some.
All inputs are finite; a program needn't handle non-finite values.
Results may differ from the reference program's by a relative error of at most 0.001.
Values may be sent and summed in bfloat16 or wider, within the bound.
A program may use at most 128 MiB of HBM per device.

```python
import jax
import jax.numpy as jnp
from jax import lax

D = 4096
HEADS = 8
HD = 128
TILE = 128
TPD = 16
KV = 1024
TILES = 512
ROWS = 65536
N_GX = 32


def draw_deal(key, part):
    inner = jax.random.fold_in(key, 7)
    first_key, second_key = jax.random.split(inner)
    base = jax.random.permutation(first_key, N_GX)
    shuffled = jax.random.permutation(second_key, N_GX)
    slot_index = jnp.arange(TPD, dtype=jnp.int32)
    offsets = shuffled[slot_index % N_GX]
    column = jnp.arange(N_GX, dtype=jnp.int32)[:, None]
    source_device = base[(column + offsets[None, :]) % N_GX]
    return (source_device * TPD + slot_index[None, :]).astype(jnp.int32)


def with_ends(drawn, own_key, least, top_value):
    dims = drawn.shape
    spot = [jax.random.randint(jax.random.fold_in(own_key, axis), (), 0, dims[axis]) for axis in range(len(dims))]
    drawn = drawn.at[tuple(spot)].set(least)
    longest = dims.index(max(dims))
    spot[longest] = (spot[longest] + 1) % dims[longest]
    return drawn.at[tuple(spot)].set(top_value)


def shard_levels(own_key, shape, cuts, smallest, top_value):
    loudness, own = 1.0, jax.random.fold_in(own_key, 6)
    for dim, blocks in cuts:
        steps = jnp.exp(jax.random.uniform(jax.random.fold_in(own, dim), (blocks,), jnp.float32, smallest / len(cuts), top_value / len(cuts)))
        loudness = loudness * jnp.repeat(steps, shape[dim] // blocks).reshape([-1 if axis == dim else 1 for axis in range(len(shape))])
    return loudness


def scatter_about(stream_key, dims, deviation, reach, shards=(), kind=jnp.bfloat16):
    gain = shard_levels(stream_key, dims, shards, -0.22, 0.18) if shards else 1.0
    result = jax.random.normal(stream_key, dims, jnp.float32) * deviation * gain
    return jnp.minimum(jnp.maximum(result, -reach), reach).astype(kind)


def setup_inputs(seed: int = 0) -> dict:
    keys = jax.random.split(jax.random.key(seed), 6)
    image_feats = scatter_about(keys[0], (ROWS, D), 1.0, 6.0, ((0, 32), (1, 8)))
    w_kv = scatter_about(keys[1], (D, 2 * KV), D ** -0.5, 0.09375, ((0, 8),))
    k_gain = jnp.clip(1.0 + 0.15 * jax.random.normal(keys[2], (HD,), jnp.float32), 0.25, 1.75)
    tile_rows = with_ends(jax.random.randint(keys[3], (TILES,), 0, TILE + 1), jax.random.fold_in(keys[3], 1), 0, TILE).astype(jnp.int32)
    deal = draw_deal(jax.random.fold_in(keys[5], 71), 0)
    return {"image_feats": image_feats, "w_kv": w_kv, "k_gain": k_gain, "tile_rows": tile_rows, "deal": deal}


epsilon = 1e-05

def reference(image_feats, w_kv, k_gain, tile_rows, deal):
    tiled = image_feats.reshape(TILES, TILE, D)
    order = deal.reshape(-1).astype(jnp.int32)
    dealt = jnp.take(tiled, order, axis=0).reshape(ROWS, D)
    projected = jnp.dot(dealt, w_kv, preferred_element_type=jnp.float32)
    projected = projected.reshape(ROWS, 2, HEADS, HD)
    key_pre = projected[:, 0]
    value_pre = projected[:, 1]
    mean_square = lax.optimization_barrier(jnp.mean(key_pre * key_pre, axis=-1, keepdims=True))
    normed = key_pre * lax.rsqrt(mean_square + epsilon) * k_gain
    limits = jnp.take(tile_rows, order, axis=0)
    position = jnp.arange(TILE, dtype=jnp.int32)
    valid = (position[None, :] < limits[:, None]).reshape(ROWS, 1, 1)
    keys_out = jnp.where(valid, normed, 0.0).reshape(ROWS, KV).astype(jnp.bfloat16)
    values_out = jnp.where(valid, value_pre, 0.0).reshape(ROWS, KV).astype(jnp.bfloat16)
    return (keys_out, values_out)
```

```python
import jax
import jax.numpy as jnp
from jax import lax
from jax.sharding import PartitionSpec as P

HD = 128
TILE = 128
TPD = 16


epsilon = 1e-05


def local(image_feats, w_kv, k_gain, tile_rows, deal):
    groups = lax.axis_size("gx")
    own_index = lax.axis_index("gx")
    slot_index = jnp.arange(TPD, dtype=jnp.int32)
    own_tiles = own_index * TPD + slot_index
    row_count = TPD * TILE
    total_kv = w_kv.shape[1] // 2
    partial_value = jnp.dot(image_feats, w_kv, preferred_element_type=jnp.float32)
    projected = lax.psum_scatter(
        partial_value.reshape(row_count, 2, total_kv), "gy", scatter_dimension=2, tiled=True
    )
    share = projected.shape[2]
    key_pre = projected[:, 0, :].reshape(row_count, share // HD, HD)
    value_pre = projected[:, 1, :]
    mean_square = jnp.mean(key_pre * key_pre, axis=-1, keepdims=True)
    normed = (key_pre * lax.rsqrt(mean_square + epsilon) * k_gain).reshape(row_count, share)
    limits = lax.dynamic_slice_in_dim(tile_rows, own_index * TPD, TPD)
    position = jnp.arange(TILE, dtype=jnp.int32)
    valid_rows = (position[None, :] < limits[:, None]).reshape(row_count, 1)
    keys = jnp.where(valid_rows, normed, 0.0).astype(jnp.bfloat16)
    values = jnp.where(valid_rows, value_pre, 0.0).astype(jnp.bfloat16)
    tiles = jnp.concatenate([keys, values], axis=1).reshape(TPD, TILE, 2 * share)
    sending = (deal == own_tiles[None, :]).astype(jnp.bfloat16)
    outgoing = jnp.einsum("ds,str->dtr", sending, tiles, preferred_element_type=jnp.float32).astype(jnp.bfloat16)
    incoming = lax.all_to_all(outgoing, "gx", split_axis=0, concat_axis=0, tiled=True)
    wanted = lax.dynamic_index_in_dim(deal, own_index, 0, keepdims=False)
    sources = jnp.arange(groups, dtype=jnp.int32)
    taking = ((wanted // TPD)[:, None] == sources[None, :]).astype(jnp.bfloat16)
    mine = jnp.einsum("sn,ntr->str", taking, incoming, preferred_element_type=jnp.float32).astype(jnp.bfloat16)
    mine = mine.reshape(row_count, 2 * share)
    return (mine[:, :share], mine[:, share:])


def solution(mesh):
    placed = (P("gx", "gy"), P("gy", None), P(), P(), P())
    return jax.shard_map(
        local, mesh=mesh, in_specs=placed, out_specs=(P("gx", "gy"), P("gx", "gy")), check_vma=False
    )
```

```python
import functools

import jax
import jax.numpy as jnp
from jax import lax
from jax.experimental import pallas as pl
from jax.experimental.pallas import tpu as pltpu
from jax.sharding import PartitionSpec as P

HD = 128
EPSILON = 1e-05
CHUNKS = 8
MESH = pl.DeviceIdType.MESH


def offsets(nz, ny):
    pairs = [(dz, dy) for dz in range(nz) for dy in range(ny) if (dz, dy) != (0, 0)]
    near = lambda d, n: min(d, n - d)
    return sorted(pairs, key=lambda p: (-near(p[0], nz) - near(p[1], ny), p[0], p[1]))


def kernel(
    nz, ny, tpd, tile, chunks,
    x_ref, w_ref, gain_ref, rows_ref, deal_ref, k_ref, v_ref,
    wv, xo, xr, keep, ps, pr, rs, rr, tiles, sb, rb, table,
    w_local, w_send, w_recv, x_local, x_send, x_recv,
    p_send, p_recv, r_send, r_recv, d_send, d_recv,
):
    groups = nz * ny
    rows = tile // chunks
    feats = x_ref.shape[2]
    total_kv = w_ref.shape[1] // 2
    gx, gy = lax.axis_index("gx"), lax.axis_index("gy")
    z, y = gx // ny, lax.rem(gx, ny)
    chip, core = gy // 2, lax.rem(gy, 2)
    mate = chip + 1 - 2 * lax.rem(chip, 2)
    across = 3 - chip
    sibling_id = (gx, chip * 2 + 1 - core)
    mate_id = (gx, mate * 2 + core)
    across_id = (gx, across * 2 + core)

    def owners(which, its_core):
        return (
            which * 2 + its_core, (3 - which) * 2 + its_core,
            which * 2 + 1 - its_core, (3 - which) * 2 + 1 - its_core,
        )

    def columns(owner, part):
        return pl.ds(pl.multiple_of(owner * HD + part * total_kv, HD), HD)

    def peer(dz, dy):
        return lax.rem(z + dz, nz) * ny + lax.rem(y + dy, ny)

    def remote(src, dst, send, recv, device):
        return pltpu.make_async_remote_copy(
            src_ref=src, dst_ref=dst, send_sem=send, recv_sem=recv, device_id=device, device_id_type=MESH
        )

    for block, owner in enumerate(owners(chip, core)):
        for part in range(2):
            pltpu.make_async_copy(
                w_ref.at[:, columns(owner, part)],
                wv.at[pl.ds(0, feats), pl.ds((2 * block + part) * HD, HD)],
                w_local,
            ).start()
    for q in range(chunks):
        pltpu.make_async_copy(x_ref.at[:, pl.ds(q * rows, rows), :], xo.at[q], x_local.at[q]).start()

    barrier = pltpu.get_barrier_semaphore()
    spread = offsets(nz, ny)
    for device in (sibling_id, mate_id, across_id):
        pl.semaphore_signal(barrier, inc=1, device_id=device, device_id_type=MESH)
    for dz, dy in spread:
        pl.semaphore_signal(barrier, inc=1, device_id=(peer(dz, dy), gy), device_id_type=MESH)
    pl.semaphore_wait(barrier, 3 + len(spread))

    for block, owner in enumerate(owners(mate, core)):
        for part in range(2):
            remote(
                w_ref.at[:, columns(owner, part)],
                wv.at[pl.ds(feats, feats), pl.ds((2 * block + part) * HD, HD)],
                w_send, w_recv, mate_id,
            ).start()
    for q in range(chunks):
        remote(x_ref.at[:, pl.ds(q * rows, rows), :], xr.at[q], x_send, x_recv.at[q], mate_id).start()

    def find(d, carry):
        found = jnp.int32(0)
        for s in range(tpd):
            source = lax.div(deal_ref[d * tpd + s], jnp.int32(tpd))
            found = jnp.where(source == gx, s, found)
        table[d] = found
        return carry

    lax.fori_loop(0, groups, find, 0)

    pltpu.make_async_copy(w_ref.at[:, pl.ds(0, 8 * HD)], wv.at[pl.ds(0, feats), :], w_local).wait()
    remote(wv.at[pl.ds(0, feats), :], wv.at[pl.ds(feats, feats), :], w_send, w_recv, mate_id).wait_recv()

    count = tpd * rows
    half = 4 * HD

    def project(q):
        pltpu.make_async_copy(x_ref.at[:, pl.ds(0, rows), :], xo.at[q], x_local.at[q]).wait()
        remote(xo.at[q], xr.at[q], x_send, x_recv.at[q], mate_id).wait_recv()
        own = xo[q].reshape(count, feats)
        other = xr[q].reshape(count, feats)
        for part, ref in ((1, ps), (0, keep)):
            ref[q] = jnp.dot(
                own, wv[0:feats, part * half:(part + 1) * half], preferred_element_type=jnp.float32
            ) + jnp.dot(
                other, wv[feats:2 * feats, part * half:(part + 1) * half], preferred_element_type=jnp.float32
            )
            if part:
                remote(ps.at[q], pr.at[q], p_send, p_recv.at[q], sibling_id).start()
        remote(ps.at[q], pr.at[q], p_send, p_recv.at[q], sibling_id).wait_recv()
        rs[q] = keep[q, :, 2 * HD:] + pr[q, :, 2 * HD:]
        remote(rs.at[q], rr.at[q], r_send, r_recv.at[q], across_id).start()
        keep[q, :, :2 * HD] = keep[q, :, :2 * HD] + pr[q, :, :2 * HD]

    def finish(q):
        remote(rs.at[q], rr.at[q], r_send, r_recv.at[q], across_id).wait_recv()
        gain = gain_ref[...]
        for s in range(tpd):
            span = pl.ds(s * rows, rows)
            key_pre = keep[q, span, :HD] + rr[q, span, :HD]
            value_pre = keep[q, span, HD:2 * HD] + rr[q, span, HD:]
            mean_square = jnp.mean(key_pre * key_pre, axis=-1, keepdims=True)
            normed = key_pre * lax.rsqrt(mean_square + EPSILON) * gain
            position = lax.broadcasted_iota(jnp.int32, (rows, HD), 0) + q * rows
            valid = position < rows_ref[gx * tpd + s]
            tiles[s, :, :HD] = jnp.where(valid, normed, 0.0).astype(jnp.bfloat16)
            tiles[s, :, HD:] = jnp.where(valid, value_pre, 0.0).astype(jnp.bfloat16)

        def fill(d, carry):
            sb[q, d] = tiles[table[d]]
            return carry

        lax.fori_loop(0, groups, fill, 0)
        place = pl.ds(pl.multiple_of(q * rows, rows), rows)
        rb[gx, place, :] = tiles[table[gx]]
        for dz, dy in spread:
            target = peer(dz, dy)
            remote(sb.at[q, target], rb.at[gx, place, :], d_send, d_recv, (target, gy)).start()

    def step(i, carry):
        @pl.when(i < chunks)
        def _():
            project(i)

        @pl.when(i >= 1)
        def _():
            finish(i - 1)

        return carry

    lax.fori_loop(0, chunks + 1, step, 0)

    far = peer(*spread[0])
    remote(sb.at[:, pl.ds(0, groups - 1)], rb.at[pl.ds(0, groups - 1)], d_send, d_recv, (far, gy)).wait_recv()
    for s in range(tpd):
        source = lax.div(deal_ref[gx * tpd + s], jnp.int32(tpd))
        k_ref[s] = rb[source, :, :HD]
        v_ref[s] = rb[source, :, HD:]

    remote(wv.at[pl.ds(0, feats), :], wv.at[pl.ds(feats, feats), :], w_send, w_recv, mate_id).wait_send()
    remote(xo, xr, x_send, x_recv.at[0], mate_id).wait_send()
    remote(ps, pr, p_send, p_recv.at[0], sibling_id).wait_send()
    remote(rs, rr, r_send, r_recv.at[0], across_id).wait_send()
    remote(sb.at[:, pl.ds(0, groups - 1)], rb.at[pl.ds(0, groups - 1)], d_send, d_recv, (far, gy)).wait_send()


def local(nz, ny, tpd, tile, chunks, image_feats, w_kv, k_gain, tile_rows, deal):
    feats = image_feats.shape[1]
    groups = nz * ny
    rows = tile // chunks
    count = tpd * rows
    bf16, f32 = jnp.bfloat16, jnp.float32
    dma = pltpu.SemaphoreType.DMA
    any_space = pl.BlockSpec(memory_space=pltpu.HBM)
    vmem = pl.BlockSpec(memory_space=pltpu.VMEM)
    smem = pl.BlockSpec(memory_space=pltpu.SMEM)
    keys, values = pl.pallas_call(
        functools.partial(kernel, nz, ny, tpd, tile, chunks),
        out_shape=(jax.ShapeDtypeStruct((tpd, tile, HD), bf16),) * 2,
        in_specs=[any_space, any_space, vmem, smem, smem],
        out_specs=(vmem, vmem),
        scratch_shapes=[
            pltpu.VMEM((2 * feats, 8 * HD), bf16),
            pltpu.VMEM((chunks, tpd, rows, feats), bf16),
            pltpu.VMEM((chunks, tpd, rows, feats), bf16),
            pltpu.VMEM((chunks, count, 4 * HD), f32),
            pltpu.VMEM((chunks, count, 4 * HD), f32),
            pltpu.VMEM((chunks, count, 4 * HD), f32),
            pltpu.VMEM((chunks, count, 2 * HD), f32),
            pltpu.VMEM((chunks, count, 2 * HD), f32),
            pltpu.VMEM((tpd, rows, 2 * HD), bf16),
            pltpu.VMEM((chunks, groups, rows, 2 * HD), bf16),
            pltpu.VMEM((groups, tile, 2 * HD), bf16),
            pltpu.SMEM((groups,), jnp.int32),
            dma, dma, dma, dma((chunks,)), dma, dma((chunks,)),
            dma, dma((chunks,)), dma, dma((chunks,)), dma, dma,
        ],
        compiler_params=pltpu.CompilerParams(
            collective_id=0, has_side_effects=True, vmem_limit_bytes=63 * 1024 * 1024
        ),
    )(
        image_feats.reshape(tpd, tile, feats), w_kv, k_gain.reshape(1, HD),
        tile_rows, deal.reshape(-1),
    )
    return (keys.reshape(tpd * tile, HD), values.reshape(tpd * tile, HD))


def build(mesh, nz, ny, tpd, tile, chunks):
    placed = (P("gx", "gy"), P("gy", None), P(), P(), P())
    return jax.shard_map(
        functools.partial(local, nz, ny, tpd, tile, chunks),
        mesh=mesh, in_specs=placed, out_specs=(P("gx", "gy"), P("gx", "gy")), check_vma=False,
    )


def solution(mesh):
    return build(mesh, 8, 4, 16, 128, CHUNKS)
```

```python
import functools

import jax
import jax.numpy as jnp
from jax import lax
from jax.experimental import pallas as pl
from jax.experimental.pallas import tpu as pltpu
from jax.sharding import PartitionSpec as P

HD = 128
EPSILON = 1e-05
CHUNKS = 8
EARLY = 2
LAG = 2
MESH = pl.DeviceIdType.MESH


def offsets(nz, ny):
    pairs = [(dz, dy) for dz in range(nz) for dy in range(ny) if (dz, dy) != (0, 0)]
    near = lambda d, n: min(d, n - d)
    return sorted(pairs, key=lambda p: (-near(p[0], nz) - near(p[1], ny), p[0], p[1]))


def kernel(
    nz, ny, tpd, tile, chunks, early,
    x_ref, w_ref, gain_ref, rows_ref, deal_ref, k_ref, v_ref,
    wv, xo, xr, xf, xs, xd, keep, ps, pr, rs, rr, tiles, sb, rb, table,
    w_local, w_send, w_mate, w_near, w_far, x_local, x_send, x_recv, f_local, f_send, f_recv,
    p_send, p_recv, r_send, r_recv, d_send, d_recv,
):
    groups = nz * ny
    rows = tile // chunks
    late = chunks - early
    late_rows, early_rows = late * rows, early * rows
    feats = x_ref.shape[2]
    total_kv = w_ref.shape[1] // 2
    tpu = tpd // 2
    count = tpu * rows
    units = 2 * chunks
    late_units = 2 * late
    gx, gy = lax.axis_index("gx"), lax.axis_index("gy")
    z, y = gx // ny, lax.rem(gx, ny)
    chip, core = gy // 2, lax.rem(gy, 2)
    mate = chip + 1 - 2 * lax.rem(chip, 2)
    across = 3 - chip
    sibling_id = (gx, chip * 2 + 1 - core)
    mate_id = (gx, mate * 2 + core)
    across_id = (gx, across * 2 + core)

    def owners(which, its_core):
        return (
            which * 2 + its_core, (3 - which) * 2 + its_core,
            which * 2 + 1 - its_core, (3 - which) * 2 + 1 - its_core,
        )

    def columns(owner, part):
        return pl.ds(pl.multiple_of(owner * HD + part * total_kv, HD), HD)

    def peer(dz, dy):
        return lax.rem(z + dz, nz) * ny + lax.rem(y + dy, ny)

    def remote(src, dst, send, recv, device):
        return pltpu.make_async_remote_copy(
            src_ref=src, dst_ref=dst, send_sem=send, recv_sem=recv, device_id=device, device_id_type=MESH
        )

    for block, owner in enumerate(owners(chip, core)):
        for part in range(2):
            pltpu.make_async_copy(
                w_ref.at[:, columns(owner, part)],
                wv.at[pl.ds(0, feats), pl.ds((2 * block + part) * HD, HD)],
                w_local,
            ).start()
    pltpu.make_async_copy(x_ref.at[:, pl.ds(late_rows, early_rows), :], xf, f_local).start()
    for u in range(late_units):
        pltpu.make_async_copy(
            x_ref.at[pl.ds(u % 2 * tpu, tpu), pl.ds(u // 2 * rows, rows), :], xo.at[u], x_local.at[u]
        ).start()

    barrier = pltpu.get_barrier_semaphore()
    spread = offsets(nz, ny)
    for device in (sibling_id, mate_id, across_id):
        pl.semaphore_signal(barrier, inc=1, device_id=device, device_id_type=MESH)
    for dz, dy in spread:
        pl.semaphore_signal(barrier, inc=1, device_id=(peer(dz, dy), gy), device_id_type=MESH)

    def find(d, carry):
        found = jnp.int32(0)
        for s in range(tpd):
            source = lax.div(deal_ref[s, d], jnp.int32(tpd))
            found = jnp.where(source == gx, s, found)
        table[d] = found
        return carry

    lax.fori_loop(0, groups, find, 0)
    pltpu.make_async_copy(x_ref.at[:, pl.ds(late_rows, early_rows), :], xf, f_local).wait()

    def gather(d, carry):
        xs[d] = xf[table[d]]
        return carry

    lax.fori_loop(0, groups, gather, 0)
    xd[gx] = xf[table[gx]]
    pl.semaphore_wait(barrier, 3 + len(spread))

    quarter = feats // ny
    part_rows = quarter // 2

    def share(owner_y, half):
        at = pl.multiple_of(feats + owner_y * quarter + half * part_rows, part_rows)
        return wv.at[pl.ds(at, part_rows), :]

    for half in range(2):
        source = pl.ds(pl.multiple_of(y * quarter + half * part_rows, part_rows), part_rows)
        at = pl.ds(pl.multiple_of(feats + y * quarter + half * part_rows, part_rows), part_rows)
        for block, owner in enumerate(owners(mate, core)):
            for part in range(2):
                remote(
                    w_ref.at[source, columns(owner, part)],
                    wv.at[at, pl.ds((2 * block + part) * HD, HD)],
                    w_send, w_mate.at[half], mate_id,
                ).start()
    for u in range(late_units):
        remote(
            x_ref.at[pl.ds(u % 2 * tpu, tpu), pl.ds(u // 2 * rows, rows), :],
            xr.at[u], x_send, x_recv.at[u], mate_id,
        ).start()
    for dz, dy in spread:
        if dy == 0:
            target = peer(dz, dy)
            remote(xs.at[target], xd.at[gx], f_send, f_recv, (target, gy)).start()

    up, down = lax.rem(y + 1, ny), lax.rem(y + ny - 1, ny)
    up_id, down_id = (z * ny + up, gy), (z * ny + down, gy)
    for half in range(2):
        remote(share(y, half), share(y, half), w_send, w_mate.at[half], mate_id).wait_recv()
        remote(share(y, half), share(y, half), w_send, w_near.at[0, half], up_id).start()
        remote(share(y, half), share(y, half), w_send, w_near.at[1, half], down_id).start()
    remote(share(down, 0), share(down, 0), w_send, w_near.at[0, 0], up_id).wait_recv()
    remote(share(down, 0), share(down, 0), w_send, w_far.at[0], up_id).start()
    remote(share(up, 1), share(up, 1), w_send, w_near.at[1, 1], down_id).wait_recv()
    remote(share(up, 1), share(up, 1), w_send, w_far.at[1], down_id).start()
    for dz, dy in spread:
        if dy != 0:
            target = peer(dz, dy)
            remote(xs.at[target], xd.at[gx], f_send, f_recv, (target, gy)).start()
    opposite = lax.rem(y + 2, ny)
    remote(share(up, 0), share(up, 0), w_send, w_near.at[1, 0], down_id).wait_recv()
    remote(share(down, 1), share(down, 1), w_send, w_near.at[0, 1], up_id).wait_recv()
    remote(share(opposite, 0), share(opposite, 0), w_send, w_far.at[0], up_id).wait_recv()
    remote(share(opposite, 1), share(opposite, 1), w_send, w_far.at[1], down_id).wait_recv()
    pltpu.make_async_copy(w_ref.at[:, pl.ds(0, 8 * HD)], wv.at[pl.ds(0, feats), :], w_local).wait()

    far = peer(*spread[0])
    half_cols = 4 * HD

    def project(u):
        @pl.when(u < late_units)
        def _():
            pltpu.make_async_copy(x_ref.at[pl.ds(0, tpu), pl.ds(0, rows), :], xo.at[u], x_local.at[u]).wait()

        remote(xo.at[u], xr.at[u], x_send, x_recv.at[u], mate_id).wait_recv()
        own = xo[u].reshape(count, feats)
        other = xr[u].reshape(count, feats)
        for part, ref in ((1, ps), (0, keep)):
            ref[u] = jnp.dot(
                own, wv[0:feats, part * half_cols:(part + 1) * half_cols], preferred_element_type=jnp.float32
            ) + jnp.dot(
                other, wv[feats:2 * feats, part * half_cols:(part + 1) * half_cols],
                preferred_element_type=jnp.float32,
            )
            if part:
                remote(ps.at[u], pr.at[u], p_send, p_recv.at[u], sibling_id).start()
        remote(ps.at[u], pr.at[u], p_send, p_recv.at[u], sibling_id).wait_recv()
        rs[u] = keep[u, :, 2 * HD:] + pr[u, :, 2 * HD:]
        remote(rs.at[u], rr.at[u], r_send, r_recv.at[u], across_id).start()
        keep[u, :, :2 * HD] = keep[u, :, :2 * HD] + pr[u, :, :2 * HD]

    def normalize(u, store):
        q, h = lax.div(u, 2), lax.rem(u, 2)
        remote(rs.at[u], rr.at[u], r_send, r_recv.at[u], across_id).wait_recv()
        gain = gain_ref[...]
        for s in range(tpu):
            span = pl.ds(s * rows, rows)
            key_pre = keep[u, span, :HD] + rr[u, span, :HD]
            value_pre = keep[u, span, HD:2 * HD] + rr[u, span, HD:]
            mean_square = jnp.mean(key_pre * key_pre, axis=-1, keepdims=True)
            normed = key_pre * lax.rsqrt(mean_square + EPSILON) * gain
            position = lax.broadcasted_iota(jnp.int32, (rows, HD), 0) + q * rows
            store(h * tpu + s, position, normed, value_pre)

    def finish_late(u):
        q = lax.div(u, 2)

        def store(s, position, normed, value_pre):
            valid = position < rows_ref[gx * tpd + s]
            tiles[s, :, :HD] = jnp.where(valid, normed, 0.0).astype(jnp.bfloat16)
            tiles[s, :, HD:] = jnp.where(valid, value_pre, 0.0).astype(jnp.bfloat16)

        normalize(u, store)

        @pl.when(lax.rem(u, 2) == 1)
        def _():
            def fill(d, carry):
                sb[q, d] = tiles[table[d]]
                return carry

            lax.fori_loop(0, groups, fill, 0)
            place = pl.ds(pl.multiple_of(q * rows, rows), rows)
            rb[gx, place, :] = tiles[table[gx]]
            for dz, dy in spread:
                target = peer(dz, dy)
                remote(sb.at[q, target], rb.at[gx, place, :], d_send, d_recv, (target, gy)).start()

    def finish_early(u):
        place = pl.ds(pl.multiple_of(lax.div(u, 2) * rows, rows), rows)

        def store(s, position, normed, value_pre):
            valid = position < rows_ref[deal_ref[s, gx]]
            k_ref[s, place, :] = jnp.where(valid, normed, 0.0).astype(jnp.bfloat16)
            v_ref[s, place, :] = jnp.where(valid, value_pre, 0.0).astype(jnp.bfloat16)

        normalize(u, store)

    def take_early():
        remote(xs.at[pl.ds(0, groups - 1)], xd.at[pl.ds(0, groups - 1)], f_send, f_recv, (far, gy)).wait_recv()
        for s in range(tpd):
            source = lax.div(deal_ref[s, gx], jnp.int32(tpd))
            for e in range(early):
                xo[late_units + 2 * e + s // tpu, s % tpu] = xd[source, e * rows:(e + 1) * rows, :]
        for u in range(late_units, units):
            remote(xo.at[u], xr.at[u], x_send, x_recv.at[u], mate_id).start()

    def step(i, carry):
        @pl.when(i < units)
        def _():
            project(i)

        @pl.when(i == max(late_units - 3, 0))
        def _():
            take_early()

        @pl.when((i >= LAG) & (i < late_units + LAG))
        def _():
            finish_late(i - LAG)

        @pl.when(i >= late_units + LAG)
        def _():
            finish_early(i - LAG)

        return carry

    lax.fori_loop(0, units + LAG, step, 0)

    remote(sb.at[:, pl.ds(0, groups - 1)], rb.at[pl.ds(0, groups - 1)], d_send, d_recv, (far, gy)).wait_recv()
    for s in range(tpd):
        source = lax.div(deal_ref[s, gx], jnp.int32(tpd))
        k_ref[s, 0:late_rows, :] = rb[source, :, :HD]
        v_ref[s, 0:late_rows, :] = rb[source, :, HD:]

    remote(wv.at[pl.ds(0, feats), :], wv.at[pl.ds(0, feats), :], w_send, w_mate.at[0], mate_id).wait_send()
    remote(xo, xr, x_send, x_recv.at[0], mate_id).wait_send()
    remote(xs.at[pl.ds(0, groups - 1)], xd.at[pl.ds(0, groups - 1)], f_send, f_recv, (far, gy)).wait_send()
    remote(ps, pr, p_send, p_recv.at[0], sibling_id).wait_send()
    remote(rs, rr, r_send, r_recv.at[0], across_id).wait_send()
    remote(sb.at[:, pl.ds(0, groups - 1)], rb.at[pl.ds(0, groups - 1)], d_send, d_recv, (far, gy)).wait_send()


def local(nz, ny, tpd, tile, chunks, early, image_feats, w_kv, k_gain, tile_rows, deal):
    feats = image_feats.shape[1]
    groups = nz * ny
    rows = tile // chunks
    units = 2 * chunks
    late = chunks - early
    count = tpd // 2 * rows
    bf16, f32 = jnp.bfloat16, jnp.float32
    dma = pltpu.SemaphoreType.DMA
    any_space = pl.BlockSpec(memory_space=pltpu.HBM)
    vmem = pl.BlockSpec(memory_space=pltpu.VMEM)
    smem = pl.BlockSpec(memory_space=pltpu.SMEM)
    keys, values = pl.pallas_call(
        functools.partial(kernel, nz, ny, tpd, tile, chunks, early),
        out_shape=(jax.ShapeDtypeStruct((tpd, tile, HD), bf16),) * 2,
        in_specs=[any_space, any_space, vmem, smem, smem],
        out_specs=(vmem, vmem),
        scratch_shapes=[
            pltpu.VMEM((2 * feats, 8 * HD), bf16),
            pltpu.VMEM((units, tpd // 2, rows, feats), bf16),
            pltpu.VMEM((units, tpd // 2, rows, feats), bf16),
            pltpu.VMEM((tpd, early * rows, feats), bf16),
            pltpu.VMEM((groups, early * rows, feats), bf16),
            pltpu.VMEM((groups, early * rows, feats), bf16),
            pltpu.VMEM((units, count, 4 * HD), f32),
            pltpu.VMEM((units, count, 4 * HD), f32),
            pltpu.VMEM((units, count, 4 * HD), f32),
            pltpu.VMEM((units, count, 2 * HD), f32),
            pltpu.VMEM((units, count, 2 * HD), f32),
            pltpu.VMEM((tpd, rows, 2 * HD), bf16),
            pltpu.VMEM((late, groups, rows, 2 * HD), bf16),
            pltpu.VMEM((groups, late * rows, 2 * HD), bf16),
            pltpu.SMEM((groups,), jnp.int32),
            dma, dma, dma((2,)), dma((2, 2)), dma((2,)),
            dma((2 * late,)), dma, dma((units,)), dma, dma, dma,
            dma, dma((units,)), dma, dma((units,)), dma, dma,
        ],
        compiler_params=pltpu.CompilerParams(
            collective_id=0, has_side_effects=True, vmem_limit_bytes=63 * 1024 * 1024
        ),
    )(image_feats.reshape(tpd, tile, feats), w_kv, k_gain.reshape(1, HD), tile_rows, deal.T)
    return (keys.reshape(tpd * tile, HD), values.reshape(tpd * tile, HD))


def build(mesh, nz, ny, tpd, tile, chunks, early=EARLY):
    placed = (P("gx", "gy"), P("gy", None), P(), P(), P())
    return jax.shard_map(
        functools.partial(local, nz, ny, tpd, tile, chunks, early),
        mesh=mesh, in_specs=placed, out_specs=(P("gx", "gy"), P("gx", "gy")), check_vma=False,
    )


def solution(mesh):
    return build(mesh, 8, 4, 16, 128, CHUNKS)
```

```python
import functools

import jax
import jax.numpy as jnp
from jax import lax
from jax.experimental import pallas as pl
from jax.experimental.pallas import tpu as pltpu
from jax.sharding import PartitionSpec as P

HD = 128
EPSILON = 1e-05
CHUNKS = 8
EARLY = 2
LAG = 2
MESH = pl.DeviceIdType.MESH


def offsets(nz, ny):
    pairs = [(dz, dy) for dz in range(nz) for dy in range(ny) if (dz, dy) != (0, 0)]
    near = lambda d, n: min(d, n - d)
    return sorted(pairs, key=lambda p: (-near(p[0], nz) - near(p[1], ny), p[0], p[1]))


def kernel(
    nz, ny, tpd, tile, chunks, early,
    x_ref, w_ref, gain_ref, rows_ref, deal_ref, k_ref, v_ref,
    wv, ws, xo, xr, xf, xs, xd, keep, ps, pr, rs, rr, tiles, sb, rb, table, rounds,
    w_local, s_local, w_send, w_mate, w_y, w_z, x_local, x_send, x_recv, f_local, f_send, f_recv,
    p_send, p_recv, r_send, r_recv, d_send, d_recv,
):
    groups = nz * ny
    rows = tile // chunks
    late = chunks - early
    late_rows, early_rows = late * rows, early * rows
    feats = x_ref.shape[2]
    total_kv = w_ref.shape[1] // 2
    tpu = tpd // 2
    shift = tpd.bit_length() - 1
    count = tpu * rows
    units = 2 * chunks
    late_units = 2 * late
    gx, gy = lax.axis_index("gx"), lax.axis_index("gy")
    z, y = gx // ny, lax.rem(gx, ny)
    chip, core = gy // 2, lax.rem(gy, 2)
    mate = chip + 1 - 2 * lax.rem(chip, 2)
    across = 3 - chip
    sibling_id = (gx, chip * 2 + 1 - core)
    mate_id = (gx, mate * 2 + core)
    across_id = (gx, across * 2 + core)

    def owners(which, its_core):
        return (
            which * 2 + its_core, (3 - which) * 2 + its_core,
            which * 2 + 1 - its_core, (3 - which) * 2 + 1 - its_core,
        )

    def columns(owner, part):
        return pl.ds(pl.multiple_of(owner * HD + part * total_kv, HD), HD)

    def peer(dz, dy):
        return lax.rem(z + dz, nz) * ny + lax.rem(y + dy, ny)

    def remote(src, dst, send, recv, device):
        return pltpu.make_async_remote_copy(
            src_ref=src, dst_ref=dst, send_sem=send, recv_sem=recv, device_id=device, device_id_type=MESH
        )

    colour = lax.rem(y + 2 * z, 4)
    quarter = feats // 4
    piece = quarter // 4
    for block, (owner, sent) in enumerate(zip(owners(chip, core), owners(mate, core))):
        for part in range(2):
            at = pl.ds((2 * block + part) * HD, HD)
            pltpu.make_async_copy(
                w_ref.at[pl.ds(pl.multiple_of(colour * quarter, quarter), quarter), columns(sent, part)],
                ws.at[:, at], s_local,
            ).start()
            pltpu.make_async_copy(w_ref.at[:, columns(owner, part)], wv.at[pl.ds(0, feats), at], w_local).start()
    pltpu.make_async_copy(x_ref.at[:, pl.ds(late_rows, early_rows), :], xf, f_local).start()
    for u in range(late_units):
        pltpu.make_async_copy(
            x_ref.at[pl.ds(u % 2 * tpu, tpu), pl.ds(u // 2 * rows, rows), :], xo.at[u], x_local.at[u]
        ).start()

    up_id, down_id = (peer(0, 1), gy), (peer(0, ny - 1), gy)
    front_id, back_id = (peer(1, 0), gy), (peer(nz - 1, 0), gy)
    barrier = pltpu.get_barrier_semaphore()
    spread = offsets(nz, ny)
    for device in (sibling_id, mate_id, across_id, up_id, down_id, front_id, back_id):
        pl.semaphore_signal(barrier, inc=1, device_id=device, device_id_type=MESH)

    def tell(number, pair):
        for device in pair:
            pl.semaphore_signal(rounds.at[number], inc=1, device_id=device, device_id_type=MESH)

    def hear(number):
        pl.semaphore_wait(rounds.at[number], 2)

    def find(d, carry):
        found = jnp.int32(0)
        for s in range(tpd):
            source = lax.shift_right_logical(deal_ref[s, d], shift)
            found = found + jnp.where(source == gx, s, 0)
        table[d] = jnp.minimum(found, tpd - 1)
        return carry

    def gather(d, carry):
        xs[d] = xf[table[d]]
        return carry

    pltpu.make_async_copy(w_ref.at[pl.ds(0, quarter), pl.ds(0, 8 * HD)], ws, s_local).wait()
    pl.semaphore_wait(barrier, 7)

    def share(kind, start, size):
        at = feats + lax.rem(kind, 4) * quarter + start * piece
        return wv.at[pl.ds(pl.multiple_of(at, piece), size * piece), :]

    for n in range(4):
        remote(
            ws.at[pl.ds(n * piece, piece), :], share(colour, n, 1), w_send, w_mate.at[n], mate_id
        ).start()
    for u in range(late_units):
        remote(
            x_ref.at[pl.ds(u % 2 * tpu, tpu), pl.ds(u // 2 * rows, rows), :],
            xr.at[u], x_send, x_recv.at[u], mate_id,
        ).start()
    tell(0, (front_id, back_id))
    lax.fori_loop(0, groups, find, 0)
    pltpu.make_async_copy(x_ref.at[:, pl.ds(late_rows, early_rows), :], xf, f_local).wait()
    hear(0)
    tell(1, (front_id, back_id))

    def pass_on(n):
        remote(share(colour, n, 1), share(colour, n, 1), w_send, w_mate.at[n], mate_id).wait_recv()
        remote(share(colour, n, 1), share(colour, n, 1), w_send, w_y.at[0], up_id).start()
        remote(share(colour, n, 1), share(colour, n, 1), w_send, w_y.at[1], down_id).start()
        remote(
            share(colour, n, 1), share(colour, n, 1), w_send, w_z.at[n // 2], front_id if n < 2 else back_id
        ).start()

    pass_on(0)
    hear(1)
    tell(2, (front_id, back_id))
    lax.fori_loop(0, groups // 2, gather, 0)
    pass_on(1)
    hear(2)
    tell(3, (up_id, down_id))
    lax.fori_loop(groups // 2, groups, gather, 0)
    xd[gx] = xf[table[gx]]
    for dz, dy in spread:
        if dy == 0:
            target = peer(dz, dy)
            remote(xs.at[target], xd.at[gx], f_send, f_recv, (target, gy)).start()
    pass_on(2)
    hear(3)
    tell(4, (up_id, down_id))
    pass_on(3)
    hear(4)
    for dz, dy in spread:
        if dy != 0:
            target = peer(dz, dy)
            remote(xs.at[target], xd.at[gx], f_send, f_recv, (target, gy)).start()
    remote(share(colour + 3, 0, 4), share(colour + 3, 0, 4), w_send, w_y.at[0], up_id).wait_recv()
    remote(share(colour + 1, 0, 4), share(colour + 1, 0, 4), w_send, w_y.at[1], down_id).wait_recv()
    remote(share(colour + 2, 0, 2), share(colour + 2, 0, 2), w_send, w_z.at[0], front_id).wait_recv()
    remote(share(colour + 2, 2, 2), share(colour + 2, 2, 2), w_send, w_z.at[1], back_id).wait_recv()
    pltpu.make_async_copy(w_ref.at[:, pl.ds(0, 8 * HD)], wv.at[pl.ds(0, feats), :], w_local).wait()

    far = peer(*spread[0])
    half_cols = 4 * HD

    def project(u):
        @pl.when(u < late_units)
        def _():
            pltpu.make_async_copy(x_ref.at[pl.ds(0, tpu), pl.ds(0, rows), :], xo.at[u], x_local.at[u]).wait()

        remote(xo.at[u], xr.at[u], x_send, x_recv.at[u], mate_id).wait_recv()
        own = xo[u].reshape(count, feats)
        other = xr[u].reshape(count, feats)
        for part, ref in ((1, ps), (0, keep)):
            ref[u] = jnp.dot(
                own, wv[0:feats, part * half_cols:(part + 1) * half_cols], preferred_element_type=jnp.float32
            ) + jnp.dot(
                other, wv[feats:2 * feats, part * half_cols:(part + 1) * half_cols],
                preferred_element_type=jnp.float32,
            )
            if part:
                remote(ps.at[u], pr.at[u], p_send, p_recv.at[u], sibling_id).start()

    def reduce(u):
        remote(ps.at[u], pr.at[u], p_send, p_recv.at[u], sibling_id).wait_recv()
        rs[u] = keep[u, :, 2 * HD:] + pr[u, :, 2 * HD:]
        remote(rs.at[u], rr.at[u], r_send, r_recv.at[u], across_id).start()
        keep[u, :, :2 * HD] = keep[u, :, :2 * HD] + pr[u, :, :2 * HD]

    def normalize(u, store):
        q, h = lax.div(u, 2), lax.rem(u, 2)
        remote(rs.at[u], rr.at[u], r_send, r_recv.at[u], across_id).wait_recv()
        gain = gain_ref[...]
        for s in range(tpu):
            span = pl.ds(s * rows, rows)
            key_pre = keep[u, span, :HD] + rr[u, span, :HD]
            value_pre = keep[u, span, HD:2 * HD] + rr[u, span, HD:]
            mean_square = jnp.mean(key_pre * key_pre, axis=-1, keepdims=True)
            normed = key_pre * lax.rsqrt(mean_square + EPSILON) * gain
            position = lax.broadcasted_iota(jnp.int32, (rows, HD), 0) + q * rows
            store(h * tpu + s, position, normed, value_pre)

    def finish_late(u):
        q = lax.div(u, 2)

        def store(s, position, normed, value_pre):
            valid = position < rows_ref[gx * tpd + s]
            tiles[s, :, :HD] = jnp.where(valid, normed, 0.0).astype(jnp.bfloat16)
            tiles[s, :, HD:] = jnp.where(valid, value_pre, 0.0).astype(jnp.bfloat16)

        normalize(u, store)

        @pl.when(lax.rem(u, 2) == 1)
        def _():
            def fill(d, carry):
                sb[q, d] = tiles[table[d]]
                return carry

            lax.fori_loop(0, groups, fill, 0)
            place = pl.ds(pl.multiple_of(q * rows, rows), rows)
            rb[gx, place, :] = tiles[table[gx]]
            for dz, dy in spread:
                target = peer(dz, dy)
                remote(sb.at[q, target], rb.at[gx, place, :], d_send, d_recv, (target, gy)).start()

    def finish_early(u):
        place = pl.ds(pl.multiple_of(lax.div(u, 2) * rows, rows), rows)

        def store(s, position, normed, value_pre):
            valid = position < rows_ref[deal_ref[s, gx]]
            k_ref[s, place, :] = jnp.where(valid, normed, 0.0).astype(jnp.bfloat16)
            v_ref[s, place, :] = jnp.where(valid, value_pre, 0.0).astype(jnp.bfloat16)

        normalize(u, store)

    def take_early():
        remote(xs.at[pl.ds(0, groups - 1)], xd.at[pl.ds(0, groups - 1)], f_send, f_recv, (far, gy)).wait_recv()
        for s in range(tpd):
            source = lax.shift_right_logical(deal_ref[s, gx], shift)
            for e in range(early):
                xo[late_units + 2 * e + s // tpu, s % tpu] = xd[source, e * rows:(e + 1) * rows, :]
        for u in range(late_units, units):
            remote(xo.at[u], xr.at[u], x_send, x_recv.at[u], mate_id).start()

    def step(i, carry):
        @pl.when(i < units)
        def _():
            project(i)

        @pl.when((i >= LAG) & (i < late_units + LAG))
        def _():
            finish_late(i - LAG)

        @pl.when(i >= late_units + LAG)
        def _():
            finish_early(i - LAG)

        @pl.when(i < units)
        def _():
            reduce(i)

        @pl.when(i == max(late_units - 3, 0))
        def _():
            take_early()

        return carry

    lax.fori_loop(0, units + LAG, step, 0)

    remote(sb.at[:, pl.ds(0, groups - 1)], rb.at[pl.ds(0, groups - 1)], d_send, d_recv, (far, gy)).wait_recv()
    for s in range(tpd):
        source = lax.shift_right_logical(deal_ref[s, gx], shift)
        k_ref[s, 0:late_rows, :] = rb[source, :, :HD]
        v_ref[s, 0:late_rows, :] = rb[source, :, HD:]

    remote(wv.at[pl.ds(0, feats), :], wv.at[pl.ds(0, feats), :], w_send, w_mate.at[0], mate_id).wait_send()
    remote(xo, xr, x_send, x_recv.at[0], mate_id).wait_send()
    remote(xs.at[pl.ds(0, groups - 1)], xd.at[pl.ds(0, groups - 1)], f_send, f_recv, (far, gy)).wait_send()
    remote(ps, pr, p_send, p_recv.at[0], sibling_id).wait_send()
    remote(rs, rr, r_send, r_recv.at[0], across_id).wait_send()
    remote(sb.at[:, pl.ds(0, groups - 1)], rb.at[pl.ds(0, groups - 1)], d_send, d_recv, (far, gy)).wait_send()


def local(nz, ny, tpd, tile, chunks, early, image_feats, w_kv, k_gain, tile_rows, deal):
    feats = image_feats.shape[1]
    groups = nz * ny
    rows = tile // chunks
    units = 2 * chunks
    late = chunks - early
    count = tpd // 2 * rows
    bf16, f32 = jnp.bfloat16, jnp.float32
    dma = pltpu.SemaphoreType.DMA
    any_space = pl.BlockSpec(memory_space=pltpu.HBM)
    vmem = pl.BlockSpec(memory_space=pltpu.VMEM)
    smem = pl.BlockSpec(memory_space=pltpu.SMEM)
    keys, values = pl.pallas_call(
        functools.partial(kernel, nz, ny, tpd, tile, chunks, early),
        out_shape=(jax.ShapeDtypeStruct((tpd, tile, HD), bf16),) * 2,
        in_specs=[any_space, any_space, vmem, smem, smem],
        out_specs=(vmem, vmem),
        scratch_shapes=[
            pltpu.VMEM((2 * feats, 8 * HD), bf16),
            pltpu.VMEM((feats // 4, 8 * HD), bf16),
            pltpu.VMEM((units, tpd // 2, rows, feats), bf16),
            pltpu.VMEM((units, tpd // 2, rows, feats), bf16),
            pltpu.VMEM((tpd, early * rows, feats), bf16),
            pltpu.VMEM((groups, early * rows, feats), bf16),
            pltpu.VMEM((groups, early * rows, feats), bf16),
            pltpu.VMEM((units, count, 4 * HD), f32),
            pltpu.VMEM((units, count, 4 * HD), f32),
            pltpu.VMEM((units, count, 4 * HD), f32),
            pltpu.VMEM((units, count, 2 * HD), f32),
            pltpu.VMEM((units, count, 2 * HD), f32),
            pltpu.VMEM((tpd, rows, 2 * HD), bf16),
            pltpu.VMEM((late, groups, rows, 2 * HD), bf16),
            pltpu.VMEM((groups, late * rows, 2 * HD), bf16),
            pltpu.SMEM((groups,), jnp.int32),
            pltpu.SemaphoreType.REGULAR((5,)),
            dma, dma, dma, dma((4,)), dma((2,)), dma((2,)),
            dma((2 * late,)), dma, dma((units,)), dma, dma, dma,
            dma, dma((units,)), dma, dma((units,)), dma, dma,
        ],
        compiler_params=pltpu.CompilerParams(
            collective_id=0, has_side_effects=True, vmem_limit_bytes=63 * 1024 * 1024
        ),
    )(image_feats.reshape(tpd, tile, feats), w_kv, k_gain.reshape(1, HD), tile_rows, deal.T)
    return (keys.reshape(tpd * tile, HD), values.reshape(tpd * tile, HD))


def build(mesh, nz, ny, tpd, tile, chunks, early=EARLY):
    placed = (P("gx", "gy"), P("gy", None), P(), P(), P())
    return jax.shard_map(
        functools.partial(local, nz, ny, tpd, tile, chunks, early),
        mesh=mesh, in_specs=placed, out_specs=(P("gx", "gy"), P("gx", "gy")), check_vma=False,
    )


def solution(mesh):
    return build(mesh, 8, 4, 16, 128, CHUNKS)
```

```python
import functools

import jax
import jax.numpy as jnp
from jax import lax
from jax.experimental import pallas as pl
from jax.experimental.pallas import tpu as pltpu
from jax.sharding import PartitionSpec as P

HD = 128
EPSILON = 1e-05
CHUNKS = 8
EARLY = 2
LAG = 2
MESH = pl.DeviceIdType.MESH


def offsets(nz, ny):
    pairs = [(dz, dy) for dz in range(nz) for dy in range(ny) if (dz, dy) != (0, 0)]
    near = lambda d, n: min(d, n - d)
    return sorted(pairs, key=lambda p: (-near(p[0], nz) - near(p[1], ny), p[0], p[1]))


def kernel(
    nz, ny, tpd, tile, chunks, early,
    x_ref, w_ref, gain_ref, rows_ref, deal_ref, kv_ref,
    wv, ws, xo, xr, xf, xs, xd, keep, ps, pr, rs, rr, tiles, sb, rb, table, rounds,
    w_local, s_local, w_send, w_mate, w_y, w_z, x_local, x_send, x_recv, f_local, f_send, f_recv,
    p_send, p_recv, r_send, r_recv, d_send, d_recv,
):
    groups = nz * ny
    rows = tile // chunks
    late = chunks - early
    late_rows, early_rows = late * rows, early * rows
    feats = x_ref.shape[2]
    total_kv = w_ref.shape[1] // 2
    tpu = tpd // 2
    shift = tpd.bit_length() - 1
    count = tpu * rows
    units = 2 * chunks
    late_units = 2 * late
    gx, gy = lax.axis_index("gx"), lax.axis_index("gy")
    z, y = gx // ny, lax.rem(gx, ny)
    chip, core = gy // 2, lax.rem(gy, 2)
    mate = chip + 1 - 2 * lax.rem(chip, 2)
    across = 3 - chip
    sibling_id = (gx, chip * 2 + 1 - core)
    mate_id = (gx, mate * 2 + core)
    across_id = (gx, across * 2 + core)

    def owners(which, its_core):
        return (
            which * 2 + its_core, (3 - which) * 2 + its_core,
            which * 2 + 1 - its_core, (3 - which) * 2 + 1 - its_core,
        )

    def columns(owner, part):
        return pl.ds(pl.multiple_of(owner * HD + part * total_kv, HD), HD)

    def peer(dz, dy):
        return lax.rem(z + dz, nz) * ny + lax.rem(y + dy, ny)

    def remote(src, dst, send, recv, device):
        return pltpu.make_async_remote_copy(
            src_ref=src, dst_ref=dst, send_sem=send, recv_sem=recv, device_id=device, device_id_type=MESH
        )

    colour = lax.rem(y + 2 * z, 4)
    quarter = feats // 4
    piece = quarter // 4
    for block, (owner, sent) in enumerate(zip(owners(chip, core), owners(mate, core))):
        for part in range(2):
            at = pl.ds((2 * block + part) * HD, HD)
            pltpu.make_async_copy(
                w_ref.at[pl.ds(pl.multiple_of(colour * quarter, quarter), quarter), columns(sent, part)],
                ws.at[:, at], s_local,
            ).start()
            pltpu.make_async_copy(w_ref.at[:, columns(owner, part)], wv.at[pl.ds(0, feats), at], w_local).start()
    pltpu.make_async_copy(x_ref.at[:, pl.ds(late_rows, early_rows), :], xf, f_local).start()
    for u in range(late_units):
        pltpu.make_async_copy(
            x_ref.at[pl.ds(u % 2 * tpu, tpu), pl.ds(u // 2 * rows, rows), :], xo.at[u], x_local.at[u]
        ).start()

    up_id, down_id = (peer(0, 1), gy), (peer(0, ny - 1), gy)
    front_id, back_id = (peer(1, 0), gy), (peer(nz - 1, 0), gy)
    barrier = pltpu.get_barrier_semaphore()
    spread = offsets(nz, ny)
    for device in (sibling_id, mate_id, across_id, up_id, down_id, front_id, back_id):
        pl.semaphore_signal(barrier, inc=1, device_id=device, device_id_type=MESH)

    def tell(number, pair):
        for device in pair:
            pl.semaphore_signal(rounds.at[number], inc=1, device_id=device, device_id_type=MESH)

    def hear(number):
        pl.semaphore_wait(rounds.at[number], 2)

    def find(d, carry):
        found = jnp.int32(0)
        for s in range(tpd):
            source = lax.shift_right_logical(deal_ref[s, d], shift)
            found = found + jnp.where(source == gx, s, 0)
        table[d] = jnp.minimum(found, tpd - 1)
        return carry

    def gather(d, carry):
        xs[d] = xf[table[d]]
        return carry

    pltpu.make_async_copy(w_ref.at[pl.ds(0, quarter), pl.ds(0, 8 * HD)], ws, s_local).wait()
    pl.semaphore_wait(barrier, 7)

    def share(kind, start, size):
        at = feats + lax.rem(kind, 4) * quarter + start * piece
        return wv.at[pl.ds(pl.multiple_of(at, piece), size * piece), :]

    for n in range(4):
        remote(
            ws.at[pl.ds(n * piece, piece), :], share(colour, n, 1), w_send, w_mate.at[n], mate_id
        ).start()
    for u in range(late_units):
        remote(
            x_ref.at[pl.ds(u % 2 * tpu, tpu), pl.ds(u // 2 * rows, rows), :],
            xr.at[u], x_send, x_recv.at[u], mate_id,
        ).start()
    tell(0, (front_id, back_id))
    lax.fori_loop(0, groups, find, 0)
    pltpu.make_async_copy(x_ref.at[:, pl.ds(late_rows, early_rows), :], xf, f_local).wait()
    hear(0)
    tell(1, (front_id, back_id))

    def pass_on(n):
        remote(share(colour, n, 1), share(colour, n, 1), w_send, w_mate.at[n], mate_id).wait_recv()
        remote(share(colour, n, 1), share(colour, n, 1), w_send, w_y.at[0], up_id).start()
        remote(share(colour, n, 1), share(colour, n, 1), w_send, w_y.at[1], down_id).start()
        remote(
            share(colour, n, 1), share(colour, n, 1), w_send, w_z.at[n // 2], front_id if n < 2 else back_id
        ).start()

    pass_on(0)
    hear(1)
    tell(2, (front_id, back_id))
    lax.fori_loop(0, groups // 2, gather, 0)
    pass_on(1)
    hear(2)
    tell(3, (up_id, down_id))
    lax.fori_loop(groups // 2, groups, gather, 0)
    xd[gx] = xf[table[gx]]
    pass_on(2)
    hear(3)
    tell(4, (up_id, down_id))
    pass_on(3)
    hear(4)
    for dz, dy in spread:
        target = peer(dz, dy)
        remote(xs.at[target], xd.at[gx], f_send, f_recv, (target, gy)).start()
    remote(share(colour + 3, 0, 4), share(colour + 3, 0, 4), w_send, w_y.at[0], up_id).wait_recv()
    remote(share(colour + 1, 0, 4), share(colour + 1, 0, 4), w_send, w_y.at[1], down_id).wait_recv()
    remote(share(colour + 2, 0, 2), share(colour + 2, 0, 2), w_send, w_z.at[0], front_id).wait_recv()
    remote(share(colour + 2, 2, 2), share(colour + 2, 2, 2), w_send, w_z.at[1], back_id).wait_recv()
    pltpu.make_async_copy(w_ref.at[:, pl.ds(0, 8 * HD)], wv.at[pl.ds(0, feats), :], w_local).wait()

    far = peer(*spread[0])
    half_cols = 4 * HD

    def project(u):
        @pl.when(u < late_units)
        def _():
            pltpu.make_async_copy(x_ref.at[pl.ds(0, tpu), pl.ds(0, rows), :], xo.at[u], x_local.at[u]).wait()

        remote(xo.at[u], xr.at[u], x_send, x_recv.at[u], mate_id).wait_recv()
        own = xo[u].reshape(count, feats)
        other = xr[u].reshape(count, feats)
        for part, ref in ((1, ps), (0, keep)):
            ref[u] = jnp.dot(
                own, wv[0:feats, part * half_cols:(part + 1) * half_cols], preferred_element_type=jnp.float32
            ) + jnp.dot(
                other, wv[feats:2 * feats, part * half_cols:(part + 1) * half_cols],
                preferred_element_type=jnp.float32,
            )
            if part:
                remote(ps.at[u], pr.at[u], p_send, p_recv.at[u], sibling_id).start()

    def reduce(u):
        remote(ps.at[u], pr.at[u], p_send, p_recv.at[u], sibling_id).wait_recv()
        rs[u] = keep[u, :, 2 * HD:] + pr[u, :, 2 * HD:]
        remote(rs.at[u], rr.at[u], r_send, r_recv.at[u], across_id).start()
        keep[u, :, :2 * HD] = keep[u, :, :2 * HD] + pr[u, :, :2 * HD]

    def normalize(u, store):
        q, h = lax.div(u, 2), lax.rem(u, 2)
        remote(rs.at[u], rr.at[u], r_send, r_recv.at[u], across_id).wait_recv()
        gain = gain_ref[...]
        for s in range(tpu):
            span = pl.ds(s * rows, rows)
            key_pre = keep[u, span, :HD] + rr[u, span, :HD]
            value_pre = keep[u, span, HD:2 * HD] + rr[u, span, HD:]
            mean_square = jnp.mean(key_pre * key_pre, axis=-1, keepdims=True)
            normed = key_pre * lax.rsqrt(mean_square + EPSILON) * gain
            position = lax.broadcasted_iota(jnp.int32, (rows, HD), 0) + q * rows
            store(h * tpu + s, position, normed, value_pre)

    def finish_late(u):
        q = lax.div(u, 2)

        def store(s, position, normed, value_pre):
            valid = position < rows_ref[gx * tpd + s]
            tiles[s, :, :HD] = jnp.where(valid, normed, 0.0).astype(jnp.bfloat16)
            tiles[s, :, HD:] = jnp.where(valid, value_pre, 0.0).astype(jnp.bfloat16)

        normalize(u, store)

        @pl.when(lax.rem(u, 2) == 1)
        def _():
            def fill(d, carry):
                sb[q, d] = tiles[table[d]]
                return carry

            lax.fori_loop(0, groups, fill, 0)
            place = pl.ds(pl.multiple_of(q * rows, rows), rows)
            rb[gx, place, :] = tiles[table[gx]]
            for dz, dy in spread:
                target = peer(dz, dy)
                remote(sb.at[q, target], rb.at[gx, place, :], d_send, d_recv, (target, gy)).start()

    def finish_early(u):
        place = pl.ds(pl.multiple_of(lax.div(u, 2) * rows, rows), rows)

        def store(s, position, normed, value_pre):
            valid = position < rows_ref[deal_ref[s, gx]]
            kv_ref[s, place, :HD] = jnp.where(valid, normed, 0.0).astype(jnp.bfloat16)
            kv_ref[s, place, HD:] = jnp.where(valid, value_pre, 0.0).astype(jnp.bfloat16)

        normalize(u, store)

    def take_early():
        remote(xs.at[pl.ds(0, groups - 1)], xd.at[pl.ds(0, groups - 1)], f_send, f_recv, (far, gy)).wait_recv()
        for s in range(tpd):
            source = lax.shift_right_logical(deal_ref[s, gx], shift)
            for e in range(early):
                xo[late_units + 2 * e + s // tpu, s % tpu] = xd[source, e * rows:(e + 1) * rows, :]
        for u in range(late_units, units):
            remote(xo.at[u], xr.at[u], x_send, x_recv.at[u], mate_id).start()

    def step(i, carry):
        @pl.when(i < units)
        def _():
            project(i)

        @pl.when((i >= LAG) & (i < late_units + LAG))
        def _():
            finish_late(i - LAG)

        @pl.when(i >= late_units + LAG)
        def _():
            finish_early(i - LAG)

        @pl.when(i < units)
        def _():
            reduce(i)

        @pl.when(i == max(late_units - 3, 0))
        def _():
            take_early()

        return carry

    lax.fori_loop(0, units + LAG, step, 0)

    remote(sb.at[:, pl.ds(0, groups - 1)], rb.at[pl.ds(0, groups - 1)], d_send, d_recv, (far, gy)).wait_recv()
    for s in range(tpd):
        source = lax.shift_right_logical(deal_ref[s, gx], shift)
        kv_ref[s, 0:late_rows, :] = rb[source]

    remote(wv.at[pl.ds(0, feats), :], wv.at[pl.ds(0, feats), :], w_send, w_mate.at[0], mate_id).wait_send()
    remote(xo, xr, x_send, x_recv.at[0], mate_id).wait_send()
    remote(xs.at[pl.ds(0, groups - 1)], xd.at[pl.ds(0, groups - 1)], f_send, f_recv, (far, gy)).wait_send()
    remote(ps, pr, p_send, p_recv.at[0], sibling_id).wait_send()
    remote(rs, rr, r_send, r_recv.at[0], across_id).wait_send()
    remote(sb.at[:, pl.ds(0, groups - 1)], rb.at[pl.ds(0, groups - 1)], d_send, d_recv, (far, gy)).wait_send()


def local(nz, ny, tpd, tile, chunks, early, image_feats, w_kv, k_gain, tile_rows, deal):
    feats = image_feats.shape[1]
    groups = nz * ny
    rows = tile // chunks
    units = 2 * chunks
    late = chunks - early
    count = tpd // 2 * rows
    bf16, f32 = jnp.bfloat16, jnp.float32
    dma = pltpu.SemaphoreType.DMA
    any_space = pl.BlockSpec(memory_space=pltpu.HBM)
    vmem = pl.BlockSpec(memory_space=pltpu.VMEM)
    smem = pl.BlockSpec(memory_space=pltpu.SMEM)
    both = pl.pallas_call(
        functools.partial(kernel, nz, ny, tpd, tile, chunks, early),
        out_shape=jax.ShapeDtypeStruct((tpd, tile, 2 * HD), bf16),
        in_specs=[any_space, any_space, vmem, smem, smem],
        out_specs=vmem,
        scratch_shapes=[
            pltpu.VMEM((2 * feats, 8 * HD), bf16),
            pltpu.VMEM((feats // 4, 8 * HD), bf16),
            pltpu.VMEM((units, tpd // 2, rows, feats), bf16),
            pltpu.VMEM((units, tpd // 2, rows, feats), bf16),
            pltpu.VMEM((tpd, early * rows, feats), bf16),
            pltpu.VMEM((groups, early * rows, feats), bf16),
            pltpu.VMEM((groups, early * rows, feats), bf16),
            pltpu.VMEM((units, count, 4 * HD), f32),
            pltpu.VMEM((units, count, 4 * HD), f32),
            pltpu.VMEM((units, count, 4 * HD), f32),
            pltpu.VMEM((units, count, 2 * HD), f32),
            pltpu.VMEM((units, count, 2 * HD), f32),
            pltpu.VMEM((tpd, rows, 2 * HD), bf16),
            pltpu.VMEM((late, groups, rows, 2 * HD), bf16),
            pltpu.VMEM((groups, late * rows, 2 * HD), bf16),
            pltpu.SMEM((groups,), jnp.int32),
            pltpu.SemaphoreType.REGULAR((5,)),
            dma, dma, dma, dma((4,)), dma((2,)), dma((2,)),
            dma((2 * late,)), dma, dma((units,)), dma, dma, dma,
            dma, dma((units,)), dma, dma((units,)), dma, dma,
        ],
        compiler_params=pltpu.CompilerParams(
            collective_id=0, has_side_effects=True, vmem_limit_bytes=63 * 1024 * 1024
        ),
    )(image_feats.reshape(tpd, tile, feats), w_kv, k_gain.reshape(1, HD), tile_rows, deal.T)
    both = both.reshape(tpd * tile, 2 * HD)
    return (both[:, :HD], both[:, HD:])


def build(mesh, nz, ny, tpd, tile, chunks, early=EARLY):
    placed = (P("gx", "gy"), P("gy", None), P(), P(), P())
    return jax.shard_map(
        functools.partial(local, nz, ny, tpd, tile, chunks, early),
        mesh=mesh, in_specs=placed, out_specs=(P("gx", "gy"), P("gx", "gy")), check_vma=False,
    )


def solution(mesh):
    return build(mesh, 8, 4, 16, 128, CHUNKS)
```

```python
import functools

import jax
import jax.numpy as jnp
from jax import lax
from jax.experimental import pallas as pl
from jax.experimental.pallas import tpu as pltpu
from jax.sharding import PartitionSpec as P

HD = 128
EPSILON = 1e-05
CHUNKS = 8
EARLY = 2
LAG = 2
MESH = pl.DeviceIdType.MESH


def offsets(nz, ny):
    pairs = [(dz, dy) for dz in range(nz) for dy in range(ny) if (dz, dy) != (0, 0)]
    near = lambda d, n: min(d, n - d)
    return sorted(pairs, key=lambda p: (-near(p[0], nz) - near(p[1], ny), p[0], p[1]))


def kernel(
    nz, ny, tpd, tile, chunks, early,
    x_ref, w_ref, gain_ref, deal_ref, kv_ref,
    wv, ws, xo, xr, xf, xs, xd, keep, ps, pr, rs, rr, tiles, sb, rb, table, rounds,
    w_local, s_local, w_send, w_mate, w_y, w_z, x_local, x_send, x_recv, f_local, f_send, f_recv,
    p_send, p_recv, r_send, r_recv, d_send, d_recv,
):
    groups = nz * ny
    rows = tile // chunks
    late = chunks - early
    late_rows, early_rows = late * rows, early * rows
    feats = x_ref.shape[2]
    total_kv = w_ref.shape[1] // 2
    tpu = tpd // 2
    shift = tpd.bit_length() - 1
    count = tpu * rows
    units = 2 * chunks
    late_units = 2 * late
    gx, gy = lax.axis_index("gx"), lax.axis_index("gy")
    z, y = gx // ny, lax.rem(gx, ny)
    chip, core = gy // 2, lax.rem(gy, 2)
    mate = chip + 1 - 2 * lax.rem(chip, 2)
    across = 3 - chip
    sibling_id = (gx, chip * 2 + 1 - core)
    mate_id = (gx, mate * 2 + core)
    across_id = (gx, across * 2 + core)

    def owners(which, its_core):
        return (
            which * 2 + its_core, (3 - which) * 2 + its_core,
            which * 2 + 1 - its_core, (3 - which) * 2 + 1 - its_core,
        )

    def columns(owner, part):
        return pl.ds(pl.multiple_of(owner * HD + part * total_kv, HD), HD)

    def peer(dz, dy):
        return lax.rem(z + dz, nz) * ny + lax.rem(y + dy, ny)

    def remote(src, dst, send, recv, device):
        return pltpu.make_async_remote_copy(
            src_ref=src, dst_ref=dst, send_sem=send, recv_sem=recv, device_id=device, device_id_type=MESH
        )

    colour = lax.rem(y + 2 * z, 4)
    quarter = feats // 4
    piece = quarter // 4
    for block, (owner, sent) in enumerate(zip(owners(chip, core), owners(mate, core))):
        for part in range(2):
            at = pl.ds((2 * block + part) * HD, HD)
            pltpu.make_async_copy(
                w_ref.at[pl.ds(pl.multiple_of(colour * quarter, quarter), quarter), columns(sent, part)],
                ws.at[:, at], s_local,
            ).start()
            pltpu.make_async_copy(w_ref.at[:, columns(owner, part)], wv.at[pl.ds(0, feats), at], w_local).start()
    pltpu.make_async_copy(x_ref.at[:, pl.ds(late_rows, early_rows), :], xf, f_local).start()
    for u in range(late_units):
        pltpu.make_async_copy(
            x_ref.at[pl.ds(u % 2 * tpu, tpu), pl.ds(u // 2 * rows, rows), :], xo.at[u], x_local.at[u]
        ).start()

    up_id, down_id = (peer(0, 1), gy), (peer(0, ny - 1), gy)
    front_id, back_id = (peer(1, 0), gy), (peer(nz - 1, 0), gy)
    barrier = pltpu.get_barrier_semaphore()
    spread = offsets(nz, ny)
    for device in (sibling_id, mate_id, across_id, up_id, down_id, front_id, back_id):
        pl.semaphore_signal(barrier, inc=1, device_id=device, device_id_type=MESH)

    def limit_of(t):
        return deal_ref[tpd + lax.div(t, groups), lax.rem(t, groups)]

    def tell(number, pair):
        for device in pair:
            pl.semaphore_signal(rounds.at[number], inc=1, device_id=device, device_id_type=MESH)

    def hear(number):
        pl.semaphore_wait(rounds.at[number], 2)

    def find(d, carry):
        found = jnp.int32(0)
        for s in range(tpd):
            source = lax.shift_right_logical(deal_ref[s, d], shift)
            found = found + jnp.where(source == gx, s, 0)
        table[d] = jnp.minimum(found, tpd - 1)
        return carry

    def gather(d, carry):
        xs[d] = xf[table[d]]
        return carry

    pltpu.make_async_copy(w_ref.at[pl.ds(0, quarter), pl.ds(0, 8 * HD)], ws, s_local).wait()
    pl.semaphore_wait(barrier, 7)

    def share(kind, start, size):
        at = feats + lax.rem(kind, 4) * quarter + start * piece
        return wv.at[pl.ds(pl.multiple_of(at, piece), size * piece), :]

    for n in range(4):
        remote(
            ws.at[pl.ds(n * piece, piece), :], share(colour, n, 1), w_send, w_mate.at[n], mate_id
        ).start()
    for u in range(late_units):
        remote(
            x_ref.at[pl.ds(u % 2 * tpu, tpu), pl.ds(u // 2 * rows, rows), :],
            xr.at[u], x_send, x_recv.at[u], mate_id,
        ).start()
    tell(0, (front_id, back_id))
    lax.fori_loop(0, groups, find, 0)
    pltpu.make_async_copy(x_ref.at[:, pl.ds(late_rows, early_rows), :], xf, f_local).wait()
    hear(0)
    tell(1, (front_id, back_id))

    def pass_on(n):
        remote(share(colour, n, 1), share(colour, n, 1), w_send, w_mate.at[n], mate_id).wait_recv()
        remote(share(colour, n, 1), share(colour, n, 1), w_send, w_y.at[0], up_id).start()
        remote(share(colour, n, 1), share(colour, n, 1), w_send, w_y.at[1], down_id).start()
        remote(
            share(colour, n, 1), share(colour, n, 1), w_send, w_z.at[n // 2], front_id if n < 2 else back_id
        ).start()

    pass_on(0)
    hear(1)
    tell(2, (front_id, back_id))
    lax.fori_loop(0, groups // 2, gather, 0)
    pass_on(1)
    hear(2)
    tell(3, (up_id, down_id))
    lax.fori_loop(groups // 2, groups, gather, 0)
    xd[gx] = xf[table[gx]]
    pass_on(2)
    hear(3)
    tell(4, (up_id, down_id))
    pass_on(3)
    for dz, dy in spread:
        if dy == 0:
            target = peer(dz, dy)
            remote(xs.at[target], xd.at[gx], f_send, f_recv, (target, gy)).start()
    hear(4)
    for dz, dy in spread:
        if dy != 0:
            target = peer(dz, dy)
            remote(xs.at[target], xd.at[gx], f_send, f_recv, (target, gy)).start()
    remote(share(colour + 3, 0, 4), share(colour + 3, 0, 4), w_send, w_y.at[0], up_id).wait_recv()
    remote(share(colour + 1, 0, 4), share(colour + 1, 0, 4), w_send, w_y.at[1], down_id).wait_recv()
    remote(share(colour + 2, 0, 2), share(colour + 2, 0, 2), w_send, w_z.at[0], front_id).wait_recv()
    remote(share(colour + 2, 2, 2), share(colour + 2, 2, 2), w_send, w_z.at[1], back_id).wait_recv()
    pltpu.make_async_copy(w_ref.at[:, pl.ds(0, 8 * HD)], wv.at[pl.ds(0, feats), :], w_local).wait()

    far = peer(*spread[0])
    half_cols = 4 * HD

    def project(u):
        @pl.when(u < late_units)
        def _():
            pltpu.make_async_copy(x_ref.at[pl.ds(0, tpu), pl.ds(0, rows), :], xo.at[u], x_local.at[u]).wait()

        remote(xo.at[u], xr.at[u], x_send, x_recv.at[u], mate_id).wait_recv()
        own = xo[u].reshape(count, feats)
        other = xr[u].reshape(count, feats)
        for part, ref in ((1, ps), (0, keep)):
            ref[u] = jnp.dot(
                own, wv[0:feats, part * half_cols:(part + 1) * half_cols], preferred_element_type=jnp.float32
            ) + jnp.dot(
                other, wv[feats:2 * feats, part * half_cols:(part + 1) * half_cols],
                preferred_element_type=jnp.float32,
            )
            if part:
                remote(ps.at[u], pr.at[u], p_send, p_recv.at[u], sibling_id).start()

    def reduce(u):
        remote(ps.at[u], pr.at[u], p_send, p_recv.at[u], sibling_id).wait_recv()
        rs[u] = keep[u, :, 2 * HD:] + pr[u, :, 2 * HD:]
        remote(rs.at[u], rr.at[u], r_send, r_recv.at[u], across_id).start()
        keep[u, :, :2 * HD] = keep[u, :, :2 * HD] + pr[u, :, :2 * HD]

    def normalize(u, store):
        q, h = lax.div(u, 2), lax.rem(u, 2)
        remote(rs.at[u], rr.at[u], r_send, r_recv.at[u], across_id).wait_recv()
        gain = gain_ref[...]
        for s in range(tpu):
            span = pl.ds(s * rows, rows)
            key_pre = keep[u, span, :HD] + rr[u, span, :HD]
            value_pre = keep[u, span, HD:2 * HD] + rr[u, span, HD:]
            mean_square = jnp.mean(key_pre * key_pre, axis=-1, keepdims=True)
            normed = key_pre * lax.rsqrt(mean_square + EPSILON) * gain
            position = lax.broadcasted_iota(jnp.int32, (rows, HD), 0) + q * rows
            store(h * tpu + s, position, normed, value_pre)

    def finish_late(u):
        q = lax.div(u, 2)

        def store(s, position, normed, value_pre):
            valid = position < limit_of(gx * tpd + s)
            tiles[s, :, :HD] = jnp.where(valid, normed, 0.0).astype(jnp.bfloat16)
            tiles[s, :, HD:] = jnp.where(valid, value_pre, 0.0).astype(jnp.bfloat16)

        normalize(u, store)

        @pl.when(lax.rem(u, 2) == 1)
        def _():
            def fill(d, carry):
                sb[q, d] = tiles[table[d]]
                return carry

            lax.fori_loop(0, groups, fill, 0)
            place = pl.ds(pl.multiple_of(q * rows, rows), rows)
            rb[gx, place, :] = tiles[table[gx]]
            for dz, dy in spread:
                target = peer(dz, dy)
                remote(sb.at[q, target], rb.at[gx, place, :], d_send, d_recv, (target, gy)).start()

    def finish_early(u):
        place = pl.ds(pl.multiple_of(lax.div(u, 2) * rows, rows), rows)

        def store(s, position, normed, value_pre):
            valid = position < limit_of(deal_ref[s, gx])
            kv_ref[s, place, :HD] = jnp.where(valid, normed, 0.0).astype(jnp.bfloat16)
            kv_ref[s, place, HD:] = jnp.where(valid, value_pre, 0.0).astype(jnp.bfloat16)

        normalize(u, store)

    def take_early():
        remote(xs.at[pl.ds(0, groups - 1)], xd.at[pl.ds(0, groups - 1)], f_send, f_recv, (far, gy)).wait_recv()
        for s in range(tpd):
            source = lax.shift_right_logical(deal_ref[s, gx], shift)
            for e in range(early):
                xo[late_units + 2 * e + s // tpu, s % tpu] = xd[source, e * rows:(e + 1) * rows, :]
        for u in range(late_units, units):
            remote(xo.at[u], xr.at[u], x_send, x_recv.at[u], mate_id).start()

    def step(i, carry):
        @pl.when(i < units)
        def _():
            project(i)

        @pl.when((i >= LAG) & (i < late_units + LAG))
        def _():
            finish_late(i - LAG)

        @pl.when(i >= late_units + LAG)
        def _():
            finish_early(i - LAG)

        @pl.when(i < units)
        def _():
            reduce(i)

        @pl.when(i == max(late_units - 3, 0))
        def _():
            take_early()

        return carry

    lax.fori_loop(0, units + LAG, step, 0)

    remote(sb.at[:, pl.ds(0, groups - 1)], rb.at[pl.ds(0, groups - 1)], d_send, d_recv, (far, gy)).wait_recv()
    for s in range(tpd):
        source = lax.shift_right_logical(deal_ref[s, gx], shift)
        kv_ref[s, 0:late_rows, :] = rb[source]

    remote(wv.at[pl.ds(0, feats), :], wv.at[pl.ds(0, feats), :], w_send, w_mate.at[0], mate_id).wait_send()
    remote(xo, xr, x_send, x_recv.at[0], mate_id).wait_send()
    remote(xs.at[pl.ds(0, groups - 1)], xd.at[pl.ds(0, groups - 1)], f_send, f_recv, (far, gy)).wait_send()
    remote(ps, pr, p_send, p_recv.at[0], sibling_id).wait_send()
    remote(rs, rr, r_send, r_recv.at[0], across_id).wait_send()
    remote(sb.at[:, pl.ds(0, groups - 1)], rb.at[pl.ds(0, groups - 1)], d_send, d_recv, (far, gy)).wait_send()


def local(nz, ny, tpd, tile, chunks, early, image_feats, w_kv, k_gain, tile_rows, deal):
    feats = image_feats.shape[1]
    groups = nz * ny
    rows = tile // chunks
    units = 2 * chunks
    late = chunks - early
    count = tpd // 2 * rows
    bf16, f32 = jnp.bfloat16, jnp.float32
    dma = pltpu.SemaphoreType.DMA
    any_space = pl.BlockSpec(memory_space=pltpu.HBM)
    vmem = pl.BlockSpec(memory_space=pltpu.VMEM)
    smem = pl.BlockSpec(memory_space=pltpu.SMEM)
    both = pl.pallas_call(
        functools.partial(kernel, nz, ny, tpd, tile, chunks, early),
        out_shape=jax.ShapeDtypeStruct((tpd, tile, 2 * HD), bf16),
        in_specs=[any_space, any_space, vmem, smem],
        out_specs=vmem,
        scratch_shapes=[
            pltpu.VMEM((2 * feats, 8 * HD), bf16),
            pltpu.VMEM((feats // 4, 8 * HD), bf16),
            pltpu.VMEM((units, tpd // 2, rows, feats), bf16),
            pltpu.VMEM((units, tpd // 2, rows, feats), bf16),
            pltpu.VMEM((tpd, early * rows, feats), bf16),
            pltpu.VMEM((groups, early * rows, feats), bf16),
            pltpu.VMEM((groups, early * rows, feats), bf16),
            pltpu.VMEM((units, count, 4 * HD), f32),
            pltpu.VMEM((units, count, 4 * HD), f32),
            pltpu.VMEM((units, count, 4 * HD), f32),
            pltpu.VMEM((units, count, 2 * HD), f32),
            pltpu.VMEM((units, count, 2 * HD), f32),
            pltpu.VMEM((tpd, rows, 2 * HD), bf16),
            pltpu.VMEM((late, groups, rows, 2 * HD), bf16),
            pltpu.VMEM((groups, late * rows, 2 * HD), bf16),
            pltpu.SMEM((groups,), jnp.int32),
            pltpu.SemaphoreType.REGULAR((5,)),
            dma, dma, dma, dma((4,)), dma((2,)), dma((2,)),
            dma((2 * late,)), dma, dma((units,)), dma, dma, dma,
            dma, dma((units,)), dma, dma((units,)), dma, dma,
        ],
        compiler_params=pltpu.CompilerParams(
            collective_id=0, has_side_effects=True, vmem_limit_bytes=51 * 1024 * 1024
        ),
    )(image_feats.reshape(tpd, tile, feats), w_kv, k_gain.reshape(1, HD), jnp.concatenate([deal.T, tile_rows.reshape(tpd, groups)]))
    both = both.reshape(tpd * tile, 2 * HD)
    return (both[:, :HD], both[:, HD:])


def build(mesh, nz, ny, tpd, tile, chunks, early=EARLY):
    placed = (P("gx", "gy"), P("gy", None), P(), P(), P())
    return jax.shard_map(
        functools.partial(local, nz, ny, tpd, tile, chunks, early),
        mesh=mesh, in_specs=placed, out_specs=(P("gx", "gy"), P("gx", "gy")), check_vma=False,
    )


def solution(mesh):
    return build(mesh, 8, 4, 16, 128, CHUNKS)
```

```python
import functools

import jax
import jax.numpy as jnp
from jax import lax
from jax.experimental import pallas as pl
from jax.experimental.pallas import tpu as pltpu
from jax.sharding import PartitionSpec as P

HD = 128
EPSILON = 1e-05
CHUNKS = 8
EARLY = 2
LAG = 2
MESH = pl.DeviceIdType.MESH


def offsets(nz, ny):
    pairs = [(dz, dy) for dz in range(nz) for dy in range(ny) if (dz, dy) != (0, 0)]
    near = lambda d, n: min(d, n - d)
    return sorted(pairs, key=lambda p: (-near(p[0], nz) - near(p[1], ny), p[0], p[1]))


def kernel(
    nz, ny, tpd, tile, chunks, early,
    x_ref, w_ref, gain_ref, deal_ref, kv_ref,
    wv, ws, xo, xr, xf, xs, xd, keep, ps, pr, rs, rr, tiles, sb, rb, table, rounds,
    w_local, s_local, w_send, w_mate, w_y, w_z, x_local, x_send, x_recv, f_local, f_send, f_recv,
    p_send, p_recv, r_send, r_recv, d_send, d_recv,
):
    groups = nz * ny
    rows = tile // chunks
    late = chunks - early
    late_rows, early_rows = late * rows, early * rows
    feats = x_ref.shape[2]
    total_kv = w_ref.shape[1] // 2
    tpu = tpd // 2
    shift = tpd.bit_length() - 1
    count = tpu * rows
    units = 2 * chunks
    late_units = 2 * late
    gx, gy = lax.axis_index("gx"), lax.axis_index("gy")
    z, y = gx // ny, lax.rem(gx, ny)
    chip, core = gy // 2, lax.rem(gy, 2)
    mate = chip + 1 - 2 * lax.rem(chip, 2)
    across = 3 - chip
    sibling_id = (gx, chip * 2 + 1 - core)
    mate_id = (gx, mate * 2 + core)
    across_id = (gx, across * 2 + core)

    def owners(which, its_core):
        return (
            which * 2 + its_core, (3 - which) * 2 + its_core,
            which * 2 + 1 - its_core, (3 - which) * 2 + 1 - its_core,
        )

    def columns(owner, part):
        return pl.ds(pl.multiple_of(owner * HD + part * total_kv, HD), HD)

    def peer(dz, dy):
        return lax.rem(z + dz, nz) * ny + lax.rem(y + dy, ny)

    def remote(src, dst, send, recv, device):
        return pltpu.make_async_remote_copy(
            src_ref=src, dst_ref=dst, send_sem=send, recv_sem=recv, device_id=device, device_id_type=MESH
        )

    colour = lax.rem(y + 2 * z, 4)
    quarter = feats // 4
    piece = quarter // 8
    for block, (owner, sent) in enumerate(zip(owners(chip, core), owners(mate, core))):
        for part in range(2):
            at = pl.ds((2 * block + part) * HD, HD)
            pltpu.make_async_copy(
                w_ref.at[pl.ds(pl.multiple_of(colour * quarter, quarter), quarter), columns(sent, part)],
                ws.at[:, at], s_local,
            ).start()
            pltpu.make_async_copy(w_ref.at[:, columns(owner, part)], wv.at[pl.ds(0, feats), at], w_local).start()
    pltpu.make_async_copy(x_ref.at[:, pl.ds(late_rows, early_rows), :], xf, f_local).start()
    for u in range(late_units):
        pltpu.make_async_copy(
            x_ref.at[pl.ds(u % 2 * tpu, tpu), pl.ds(u // 2 * rows, rows), :], xo.at[u], x_local.at[u]
        ).start()

    up_id, down_id = (peer(0, 1), gy), (peer(0, ny - 1), gy)
    front_id, back_id = (peer(1, 0), gy), (peer(nz - 1, 0), gy)
    barrier = pltpu.get_barrier_semaphore()
    spread = offsets(nz, ny)
    for device in (sibling_id, mate_id, across_id, up_id, down_id, front_id, back_id):
        pl.semaphore_signal(barrier, inc=1, device_id=device, device_id_type=MESH)

    def limit_of(t):
        return deal_ref[tpd + lax.div(t, groups), lax.rem(t, groups)]

    def tell(number, pair):
        for device in pair:
            pl.semaphore_signal(rounds.at[number], inc=1, device_id=device, device_id_type=MESH)

    def hear(number):
        pl.semaphore_wait(rounds.at[number], 2)

    def find(d, carry):
        found = jnp.int32(0)
        for s in range(tpd):
            source = lax.shift_right_logical(deal_ref[s, d], shift)
            found = found + jnp.where(source == gx, s, 0)
        table[d] = jnp.minimum(found, tpd - 1)
        return carry

    def gather(d, carry):
        xs[d] = xf[table[d]]
        return carry

    pltpu.make_async_copy(w_ref.at[pl.ds(0, quarter), pl.ds(0, 8 * HD)], ws, s_local).wait()
    pl.semaphore_wait(barrier, 7)

    def share(kind, start, size):
        at = feats + lax.rem(kind, 4) * quarter + start * piece
        return wv.at[pl.ds(pl.multiple_of(at, piece), size * piece), :]

    for n in range(8):
        remote(
            ws.at[pl.ds(n * piece, piece), :], share(colour, n, 1), w_send, w_mate.at[n], mate_id
        ).start()
    for u in range(late_units):
        remote(
            x_ref.at[pl.ds(u % 2 * tpu, tpu), pl.ds(u // 2 * rows, rows), :],
            xr.at[u], x_send, x_recv.at[u], mate_id,
        ).start()
    tell(0, (front_id, back_id))
    lax.fori_loop(0, groups, find, 0)
    pltpu.make_async_copy(x_ref.at[:, pl.ds(late_rows, early_rows), :], xf, f_local).wait()
    hear(0)
    tell(1, (front_id, back_id))

    def pass_on(n):
        remote(share(colour, n, 1), share(colour, n, 1), w_send, w_mate.at[n], mate_id).wait_recv()
        remote(share(colour, n, 1), share(colour, n, 1), w_send, w_y.at[0], up_id).start()
        remote(share(colour, n, 1), share(colour, n, 1), w_send, w_y.at[1], down_id).start()
        remote(
            share(colour, n, 1), share(colour, n, 1), w_send, w_z.at[n // 4], front_id if n < 4 else back_id
        ).start()

    pass_on(0)
    pass_on(1)
    hear(1)
    tell(2, (front_id, back_id))
    lax.fori_loop(0, groups // 2, gather, 0)
    pass_on(2)
    pass_on(3)
    hear(2)
    tell(3, (up_id, down_id))
    lax.fori_loop(groups // 2, groups, gather, 0)
    xd[gx] = xf[table[gx]]
    pass_on(4)
    pass_on(5)
    hear(3)
    tell(4, (up_id, down_id))
    pass_on(6)
    pass_on(7)
    for dz, dy in spread:
        if dy == 0:
            target = peer(dz, dy)
            remote(xs.at[target], xd.at[gx], f_send, f_recv, (target, gy)).start()
    hear(4)
    for dz, dy in spread:
        if dy != 0:
            target = peer(dz, dy)
            remote(xs.at[target], xd.at[gx], f_send, f_recv, (target, gy)).start()
    remote(share(colour + 3, 0, 8), share(colour + 3, 0, 8), w_send, w_y.at[0], up_id).wait_recv()
    remote(share(colour + 1, 0, 8), share(colour + 1, 0, 8), w_send, w_y.at[1], down_id).wait_recv()
    remote(share(colour + 2, 0, 4), share(colour + 2, 0, 4), w_send, w_z.at[0], front_id).wait_recv()
    remote(share(colour + 2, 4, 4), share(colour + 2, 4, 4), w_send, w_z.at[1], back_id).wait_recv()
    pltpu.make_async_copy(w_ref.at[:, pl.ds(0, 8 * HD)], wv.at[pl.ds(0, feats), :], w_local).wait()

    far = peer(*spread[0])
    half_cols = 4 * HD

    def project(u):
        @pl.when(u < late_units)
        def _():
            pltpu.make_async_copy(x_ref.at[pl.ds(0, tpu), pl.ds(0, rows), :], xo.at[u], x_local.at[u]).wait()

        remote(xo.at[u], xr.at[u], x_send, x_recv.at[u], mate_id).wait_recv()
        own = xo[u].reshape(count, feats)
        other = xr[u].reshape(count, feats)
        for part, ref in ((1, ps), (0, keep)):
            ref[u] = jnp.dot(
                own, wv[0:feats, part * half_cols:(part + 1) * half_cols], preferred_element_type=jnp.float32
            ) + jnp.dot(
                other, wv[feats:2 * feats, part * half_cols:(part + 1) * half_cols],
                preferred_element_type=jnp.float32,
            )
            if part:
                remote(ps.at[u], pr.at[u], p_send, p_recv.at[u], sibling_id).start()

    def reduce(u):
        remote(ps.at[u], pr.at[u], p_send, p_recv.at[u], sibling_id).wait_recv()
        rs[u] = keep[u, :, 2 * HD:] + pr[u, :, 2 * HD:]
        remote(rs.at[u], rr.at[u], r_send, r_recv.at[u], across_id).start()
        keep[u, :, :2 * HD] = keep[u, :, :2 * HD] + pr[u, :, :2 * HD]

    def normalize(u, store):
        q, h = lax.div(u, 2), lax.rem(u, 2)
        remote(rs.at[u], rr.at[u], r_send, r_recv.at[u], across_id).wait_recv()
        gain = gain_ref[...]
        for s in range(tpu):
            span = pl.ds(s * rows, rows)
            key_pre = keep[u, span, :HD] + rr[u, span, :HD]
            value_pre = keep[u, span, HD:2 * HD] + rr[u, span, HD:]
            mean_square = jnp.mean(key_pre * key_pre, axis=-1, keepdims=True)
            normed = key_pre * lax.rsqrt(mean_square + EPSILON) * gain
            position = lax.broadcasted_iota(jnp.int32, (rows, HD), 0) + q * rows
            store(h * tpu + s, position, normed, value_pre)

    def finish_late(u):
        q = lax.div(u, 2)

        def store(s, position, normed, value_pre):
            valid = position < limit_of(gx * tpd + s)
            tiles[s, :, :HD] = jnp.where(valid, normed, 0.0).astype(jnp.bfloat16)
            tiles[s, :, HD:] = jnp.where(valid, value_pre, 0.0).astype(jnp.bfloat16)

        normalize(u, store)

        @pl.when(lax.rem(u, 2) == 1)
        def _():
            def fill(d, carry):
                sb[q, d] = tiles[table[d]]
                return carry

            lax.fori_loop(0, groups, fill, 0)
            place = pl.ds(pl.multiple_of(q * rows, rows), rows)
            rb[gx, place, :] = tiles[table[gx]]
            for dz, dy in spread:
                target = peer(dz, dy)
                remote(sb.at[q, target], rb.at[gx, place, :], d_send, d_recv, (target, gy)).start()

    def finish_early(u):
        place = pl.ds(pl.multiple_of(lax.div(u, 2) * rows, rows), rows)

        def store(s, position, normed, value_pre):
            valid = position < limit_of(deal_ref[s, gx])
            kv_ref[s, place, :HD] = jnp.where(valid, normed, 0.0).astype(jnp.bfloat16)
            kv_ref[s, place, HD:] = jnp.where(valid, value_pre, 0.0).astype(jnp.bfloat16)

        normalize(u, store)

    def take_early():
        remote(xs.at[pl.ds(0, groups - 1)], xd.at[pl.ds(0, groups - 1)], f_send, f_recv, (far, gy)).wait_recv()
        for s in range(tpd):
            source = lax.shift_right_logical(deal_ref[s, gx], shift)
            for e in range(early):
                xo[late_units + 2 * e + s // tpu, s % tpu] = xd[source, e * rows:(e + 1) * rows, :]
        for u in range(late_units, units):
            remote(xo.at[u], xr.at[u], x_send, x_recv.at[u], mate_id).start()

    def step(i, carry):
        @pl.when(i < units)
        def _():
            project(i)

        @pl.when((i >= LAG) & (i < late_units + LAG))
        def _():
            finish_late(i - LAG)

        @pl.when(i >= late_units + LAG)
        def _():
            finish_early(i - LAG)

        @pl.when(i < units)
        def _():
            reduce(i)

        @pl.when(i == max(late_units - 3, 0))
        def _():
            take_early()

        return carry

    lax.fori_loop(0, units + LAG, step, 0)

    remote(sb.at[:, pl.ds(0, groups - 1)], rb.at[pl.ds(0, groups - 1)], d_send, d_recv, (far, gy)).wait_recv()
    for s in range(tpd):
        source = lax.shift_right_logical(deal_ref[s, gx], shift)
        kv_ref[s, 0:late_rows, :] = rb[source]

    remote(wv.at[pl.ds(0, feats), :], wv.at[pl.ds(0, feats), :], w_send, w_mate.at[0], mate_id).wait_send()
    remote(xo, xr, x_send, x_recv.at[0], mate_id).wait_send()
    remote(xs.at[pl.ds(0, groups - 1)], xd.at[pl.ds(0, groups - 1)], f_send, f_recv, (far, gy)).wait_send()
    remote(ps, pr, p_send, p_recv.at[0], sibling_id).wait_send()
    remote(rs, rr, r_send, r_recv.at[0], across_id).wait_send()
    remote(sb.at[:, pl.ds(0, groups - 1)], rb.at[pl.ds(0, groups - 1)], d_send, d_recv, (far, gy)).wait_send()


def local(nz, ny, tpd, tile, chunks, early, image_feats, w_kv, k_gain, tile_rows, deal):
    feats = image_feats.shape[1]
    groups = nz * ny
    rows = tile // chunks
    units = 2 * chunks
    late = chunks - early
    count = tpd // 2 * rows
    bf16, f32 = jnp.bfloat16, jnp.float32
    dma = pltpu.SemaphoreType.DMA
    any_space = pl.BlockSpec(memory_space=pltpu.HBM)
    vmem = pl.BlockSpec(memory_space=pltpu.VMEM)
    smem = pl.BlockSpec(memory_space=pltpu.SMEM)
    both = pl.pallas_call(
        functools.partial(kernel, nz, ny, tpd, tile, chunks, early),
        out_shape=jax.ShapeDtypeStruct((tpd, tile, 2 * HD), bf16),
        in_specs=[any_space, any_space, vmem, smem],
        out_specs=vmem,
        scratch_shapes=[
            pltpu.VMEM((2 * feats, 8 * HD), bf16),
            pltpu.VMEM((feats // 4, 8 * HD), bf16),
            pltpu.VMEM((units, tpd // 2, rows, feats), bf16),
            pltpu.VMEM((units, tpd // 2, rows, feats), bf16),
            pltpu.VMEM((tpd, early * rows, feats), bf16),
            pltpu.VMEM((groups, early * rows, feats), bf16),
            pltpu.VMEM((groups, early * rows, feats), bf16),
            pltpu.VMEM((units, count, 4 * HD), f32),
            pltpu.VMEM((units, count, 4 * HD), f32),
            pltpu.VMEM((units, count, 4 * HD), f32),
            pltpu.VMEM((units, count, 2 * HD), f32),
            pltpu.VMEM((units, count, 2 * HD), f32),
            pltpu.VMEM((tpd, rows, 2 * HD), bf16),
            pltpu.VMEM((late, groups, rows, 2 * HD), bf16),
            pltpu.VMEM((groups, late * rows, 2 * HD), bf16),
            pltpu.SMEM((groups,), jnp.int32),
            pltpu.SemaphoreType.REGULAR((5,)),
            dma, dma, dma, dma((8,)), dma((2,)), dma((2,)),
            dma((2 * late,)), dma, dma((units,)), dma, dma, dma,
            dma, dma((units,)), dma, dma((units,)), dma, dma,
        ],
        compiler_params=pltpu.CompilerParams(
            collective_id=0, has_side_effects=True, vmem_limit_bytes=51 * 1024 * 1024
        ),
    )(image_feats.reshape(tpd, tile, feats), w_kv, k_gain.reshape(1, HD), jnp.concatenate([deal.T, tile_rows.reshape(tpd, groups)]))
    both = both.reshape(tpd * tile, 2 * HD)
    return (both[:, :HD], both[:, HD:])


def build(mesh, nz, ny, tpd, tile, chunks, early=EARLY):
    placed = (P("gx", "gy"), P("gy", None), P(), P(), P())
    return jax.shard_map(
        functools.partial(local, nz, ny, tpd, tile, chunks, early),
        mesh=mesh, in_specs=placed, out_specs=(P("gx", "gy"), P("gx", "gy")), check_vma=False,
    )


def solution(mesh):
    return build(mesh, 8, 4, 16, 128, CHUNKS)
```
